32 devices in a mesh: dp: 2 (over y), ctx: 4 (over z), tp: 4 (over x, core).
Axes of the slice: x: 2, y: 2, z: 4, core: 2. Of those that a mesh axis runs over, the one named last changes fastest.
Arguments:
- layer_input: bfloat16 [2, 512, 8192], P('dp', 'ctx'), may hold values from -6 to 6
- queries: bfloat16 [2, 512, 16384], P('dp', 'ctx', 'tp'), may hold values from -6 to 6
- key_heads: bfloat16 [2, 512, 1024], P('dp', 'ctx', 'tp'), may hold values from -6 to 6
- value_heads: bfloat16 [2, 512, 1024], P('dp', 'ctx', 'tp'), may hold values from -6 to 6
- attn_out: bfloat16 [2, 512, 16384], P('dp', 'ctx', 'tp'), may hold values from -6 to 6
- out_grad: bfloat16 [2, 512, 16384], P('dp', 'ctx', 'tp'), may hold values from -6 to 6
- log_sums: float32 [2, 128, 512], P('dp', 'tp', 'ctx'), may hold values from 4 to 7
- doc_ids: int32 [2, 512], P('dp'), may hold values from 0 to 7, never falling along the last dimension, each value on 1 to 193 neighbouring positions
Outputs:
- query_grad: bfloat16 [2, 512, 16384], P('dp', 'ctx', 'tp')
- key_grad: bfloat16 [2, 512, 1024], P('dp', 'ctx', 'tp')
- value_grad: bfloat16 [2, 512, 1024], P('dp', 'ctx', 'tp')
- weight_grad: float32 [8192, 1024], P(('dp', 'ctx'), 'tp')
The draws below stay inside these ranges and needn't reach their ends.
Inputs may be any that keep to these rules, and one draw needn't show every extreme that they name: `doc_ids`: along each sequence's positions the document ids never fall; every id names 1 to 193 positions, and one names exactly 193.
All inputs are finite; a program needn't handle non-finite values.
Results may differ from the reference program's by a relative error of at most 0.0061.
Values may be sent and summed in bfloat16 or wider, within the bound.
A program may use at most 64 MiB of HBM per device.

```python
import math
import jax
import jax.numpy as jnp
import numpy as np
from jax import lax

C = 64
REACH = 4
HQ = 128
KVH = 8
HD = 128
D = 8192
BATCH = 2
SEQ = 512
MAXDOC = 193
DOCS = 8
N_CTX = 4


def strengthened(entries, key, source, target, shards_of, factor):
    def block_of(position):
        return (jnp.arange(entries.shape[position]) // (entries.shape[position] // shards_of)).reshape((-1,) + (1,) * (entries.ndim - 1 - position))

    near = jax.random.permutation(key, shards_of)[block_of(target)]
    far = (block_of(target) + shards_of // 2) % shards_of
    return jnp.where((block_of(source) == near) | (block_of(source) == far), factor * entries, entries)


def block_scale(own_key, shape, split, low, top_value):
    loudness = 1.0
    for position, parts in split:
        steps = jax.random.uniform(jax.random.fold_in(jax.random.fold_in(own_key, 6), position), (parts,), jnp.float32, low / len(split), top_value / len(split))
        loudness = loudness * jnp.repeat(jnp.exp(steps), shape[position] // parts).reshape((-1,) + (1,) * (len(shape) - 1 - position))
    return loudness


def split_up(number_of, total, most, slope):
    loads = [(1 << 20) // math.isqrt(standing ** slope) + 1 for standing in range(2, number_of + 1)]
    rest, holding = total - most - (number_of - 1), [1] * (number_of - 1)
    while rest > 0:
        movable = [i for i in range(number_of - 1) if holding[i] < most]
        pool, left = sum([loads[i] for i in movable]), rest
        for i in movable:
            extra = min(most - holding[i], max(1, left * loads[i] // pool), rest)
            holding[i] = holding[i] + extra
            rest = rest - extra
    return np.array([most] + holding)


def ragged_sizes(stream_key, count, total, most, skew):
    if count == 2:
        one = jax.random.randint(stream_key, (), max(1, total - most), min(most, total - 1) + 1)
        return jnp.stack([one, total - one])
    lengths = jnp.asarray(split_up(count, total, most, skew), jnp.int32)
    twos = (count - 1) // 2
    giver, sink = lengths[1:1 + 2 * twos:2], lengths[2:2 + 2 * twos:2]
    room = jnp.minimum(giver - 1, most - sink)
    passed = jax.random.randint(jax.random.fold_in(stream_key, 1), (twos,), 0, 1 << 20) % (room + 1)
    lengths = lengths.at[1:1 + 2 * twos:2].set(giver - passed).at[2:2 + 2 * twos:2].set(sink + passed)
    return lengths[jax.random.permutation(jax.random.fold_in(stream_key, 2), count)]


def centred(rng, dims, spread, bound, split=(), held_as=jnp.bfloat16):
    array = spread * jax.random.normal(rng, dims, jnp.float32)
    if split:
        array = array * block_scale(rng, dims, split, -0.22, 0.18)
    return jnp.clip(array, -bound, bound).astype(held_as)


def gaussian_with(own_key, shape, deviation, bound, split, heavy, held_as=jnp.bfloat16):
    drawn = deviation * jax.random.normal(own_key, shape, jnp.float32)
    if split:
        drawn = drawn * block_scale(own_key, shape, split, -0.22, 0.18)
    return jnp.clip(strengthened(drawn, jax.random.fold_in(own_key, 3), *heavy), -bound, bound).astype(held_as)


def setup_inputs(seed: int = 0) -> dict:
    key_of = jax.random.split(jax.random.key(seed), 9)
    return {
        "layer_input": gaussian_with(key_of[0], (BATCH, SEQ, D), 1.0, 6.0, ((0, 2), (1, 4)), (1, 2, 4, 2.0)),
        "queries": centred(key_of[1], (BATCH, SEQ, HQ * HD), 1.0, 6.0, ((0, 2), (1, 4), (2, 4))),
        "key_heads": centred(key_of[2], (BATCH, SEQ, KVH * HD), 1.0, 6.0, ((0, 2), (1, 4), (2, 4))),
        "value_heads": centred(key_of[3], (BATCH, SEQ, KVH * HD), 1.0, 6.0, ((0, 2), (1, 4), (2, 4))),
        "attn_out": centred(key_of[4], (BATCH, SEQ, HQ * HD), 1.0, 6.0, ((0, 2), (1, 4), (2, 4))),
        "out_grad": centred(key_of[5], (BATCH, SEQ, HQ * HD), 1.0, 6.0, ((0, 2), (1, 4), (2, 4))),
        "log_sums": jnp.clip(4.0 + 3.0 * jax.random.uniform(key_of[6], (BATCH, HQ, SEQ), jnp.float32) ** block_scale(key_of[6], (BATCH, HQ, SEQ), ((0, 2), (1, 4), (2, 4)), -0.2, 0.2), 4.0, 7.0),
        "doc_ids": jax.vmap(lambda own: jnp.searchsorted(jnp.cumsum(ragged_sizes(own, DOCS, SEQ, MAXDOC, 1)), jnp.arange(SEQ), side="right"))(jax.random.split(key_of[7], BATCH)).reshape((BATCH, SEQ)).astype(jnp.int32),
    }


def seq_order(stored):
    blocks = stored.reshape(N_CTX, 2, C, stored.shape[-1])
    return jnp.concatenate([blocks[:, 0], blocks[::-1, 1]], axis=0)


def store_order(ordered):
    lower = ordered[:N_CTX]
    upper = ordered[N_CTX:][::-1]
    return jnp.stack([lower, upper], axis=1).reshape(SEQ, ordered.shape[-1])


def one_sequence(queries, key_heads, value_heads, attn_out, out_grad, log_sums, doc_seq):
    per_group = HQ // KVH
    score_scale = HD ** -0.5
    margin = (REACH - 1) * C
    key_span = REACH * C
    query_blocks = seq_order(queries).reshape(2 * N_CTX, C, KVH, per_group, HD)
    grad_blocks = seq_order(out_grad).reshape(2 * N_CTX, C, KVH, per_group, HD)
    out_blocks = seq_order(attn_out).reshape(2 * N_CTX, C, KVH, per_group, HD)
    lse_blocks = seq_order(log_sums.T).reshape(2 * N_CTX, C, KVH, per_group)
    pad_rows = jnp.zeros((margin, KVH * HD), jnp.bfloat16)
    key_seq = jnp.concatenate([pad_rows, seq_order(key_heads).reshape(SEQ, KVH * HD)], axis=0)
    value_seq = jnp.concatenate([pad_rows, seq_order(value_heads).reshape(SEQ, KVH * HD)], axis=0)
    doc_int = doc_seq.astype(jnp.int32)
    doc_pad = jnp.concatenate([jnp.full((margin,), -1, jnp.int32), doc_int], axis=0)
    offsets = jnp.arange(C, dtype=jnp.int32)
    key_offsets = jnp.arange(key_span, dtype=jnp.int32)

    def visit_block(running, inputs):
        grad_keys, grad_values = running
        block_index, query_rows, grad_rows, out_rows, lse_block = inputs
        start_row = block_index * C
        query_full = query_rows.astype(jnp.float32)
        grad_full = grad_rows.astype(jnp.float32)
        out_full = out_rows.astype(jnp.float32)
        key_full = lax.dynamic_slice_in_dim(key_seq, start_row, key_span, 0).astype(jnp.float32).reshape(key_span, KVH, HD)
        value_full = lax.dynamic_slice_in_dim(value_seq, start_row, key_span, 0).astype(jnp.float32).reshape(key_span, KVH, HD)
        key_doc = lax.dynamic_slice_in_dim(doc_pad, start_row, key_span, 0)
        query_doc = lax.dynamic_slice_in_dim(doc_int, start_row, C, 0)
        query_pos = start_row + offsets
        key_pos = start_row - margin + key_offsets
        live_mask = (key_pos[None, :] <= query_pos[:, None]) & (key_doc[None, :] == query_doc[:, None])
        lse_rows = lse_block.transpose(1, 2, 0)
        scores = jnp.einsum("qgrd,kgd->grqk", query_full, key_full) * score_scale
        soft_probs = jnp.where(live_mask, jnp.exp(scores - lse_rows[..., None]), 0.0)
        probs_bf = lax.optimization_barrier(soft_probs.astype(jnp.bfloat16)).astype(jnp.float32)
        grad_value = jnp.einsum("grqk,qgrd->kgd", probs_bf, grad_full)
        grad_probs = jnp.einsum("qgrd,kgd->grqk", grad_full, value_full)
        row_delta = jnp.sum(grad_full * out_full, axis=-1).transpose(1, 2, 0)
        grad_scores = lax.optimization_barrier((soft_probs * (grad_probs - row_delta[..., None])).astype(jnp.bfloat16)).astype(jnp.float32)
        grad_query = jnp.einsum("grqk,kgd->qgrd", grad_scores, key_full) * score_scale
        grad_key = jnp.einsum("grqk,qgrd->kgd", grad_scores, query_full) * score_scale
        grad_keys = lax.dynamic_update_slice_in_dim(grad_keys, lax.dynamic_slice_in_dim(grad_keys, start_row, key_span, 0) + grad_key.reshape(key_span, KVH * HD), start_row, 0)
        grad_values = lax.dynamic_update_slice_in_dim(grad_values, lax.dynamic_slice_in_dim(grad_values, start_row, key_span, 0) + grad_value.reshape(key_span, KVH * HD), start_row, 0)
        return (grad_keys, grad_values), grad_query.reshape(C, HQ * HD)

    zeros_rows = jnp.zeros((SEQ + margin, KVH * HD), jnp.float32)
    blocks = jnp.arange(2 * N_CTX, dtype=jnp.int32)
    (grad_keys, grad_values), grad_queries = lax.scan(visit_block, (zeros_rows, zeros_rows), (blocks, query_blocks, grad_blocks, out_blocks, lse_blocks))
    grad_keys = store_order(grad_keys[margin:].reshape(2 * N_CTX, C, KVH * HD))
    grad_values = store_order(grad_values[margin:].reshape(2 * N_CTX, C, KVH * HD))
    grad_queries = store_order(grad_queries)
    return grad_queries.astype(jnp.bfloat16), grad_keys.astype(jnp.bfloat16), grad_values.astype(jnp.bfloat16)


def reference(layer_input, queries, key_heads, value_heads, attn_out, out_grad, log_sums, doc_ids):
    query_list = []
    key_list = []
    value_list = []
    for batch_row in range(queries.shape[0]):
        results = one_sequence(queries[batch_row], key_heads[batch_row], value_heads[batch_row], attn_out[batch_row], out_grad[batch_row], log_sums[batch_row], doc_ids[batch_row])
        query_list.append(results[0])
        key_list.append(results[1])
        value_list.append(results[2])
    query_grad = jnp.stack(query_list, axis=0)
    key_grad = jnp.stack(key_list, axis=0)
    value_grad = jnp.stack(value_list, axis=0)
    total = jnp.zeros((layer_input.shape[2], KVH * HD), jnp.float32)
    for batch_row in range(queries.shape[0]):
        total = total + jnp.dot(layer_input[batch_row].T, value_grad[batch_row], preferred_element_type=jnp.float32)
    weight_grad = total * (queries.shape[0] * SEQ) ** -0.5
    return query_grad, key_grad, value_grad, weight_grad
```

```python
import functools
import jax
import jax.numpy as jnp
from jax import lax
from jax.experimental import pallas as pl
from jax.experimental.pallas import tpu as pltpu
from jax.sharding import PartitionSpec as P

REACH = 4
HD = 128
LANES = 128
CORES = 2
MESH = pl.DeviceIdType.MESH
F32 = jnp.float32
BF16 = jnp.bfloat16


def contract(left, right, dims):
    return lax.dot_general(left, right, (dims, ((), ())), preferred_element_type=F32)


def place_of(block, count):
    return jnp.where(block < count, block, 2 * count - 1 - block), jnp.where(block < count, 0, 1)


def fused_kernel(
    sizes,
    layer_hbm,
    q_hbm,
    k_hbm,
    v_hbm,
    o_hbm,
    do_hbm,
    lse_ref,
    doc_ref,
    dq_hbm,
    dk_ref,
    dv_ref,
    w_hbm,
    q_s,
    o_s,
    do_s,
    dq_s,
    kbuf,
    vbuf,
    bias_s,
    lse_s,
    dkv_s,
    acc_s,
    send_s,
    recv_s,
    a_s,
    at_s,
    vg_s,
    w_s,
    load_sem,
    own_sem,
    kv_send,
    kv_recv,
    g_send,
    g_recv,
    a_send,
    a_recv,
    x_send,
    x_recv,
    c_send,
    c_recv,
    vg_send,
    vg_recv,
    out_sem,
):
    ndp, n, ntp = sizes
    dp, me, tp = lax.axis_index("dp"), lax.axis_index("ctx"), lax.axis_index("tp")
    rows = q_s.shape[0]
    block = rows // 2
    groups = k_hbm.shape[2] // HD
    per_group = q_s.shape[1] // HD // groups
    stack = 2 * LANES // block
    span = REACH * block
    width = groups * HD
    scale = HD ** (-0.5)
    feats = w_s.shape[0]
    xs = ntp // CORES
    core = lax.rem(tp, CORES)
    chip = tp // CORES
    strip = rows // ntp
    own_row = pl.multiple_of((core * xs + chip) * strip, strip)
    core_row = pl.multiple_of(core * xs * strip, strip)
    others = [(a, b) for a in range(ndp) for b in range(n) if (a, b) != (0, 0)]
    others.sort(key=lambda ab: (ab[1] != 0, ab[0] + min(ab[1], n - ab[1])))
    blocks = (me, 2 * n - 1 - me)

    def peer(shift):
        return lax.rem(dp + shift[0], ndp), lax.rem(me + shift[1], n)

    def source(shift):
        return lax.rem(dp + ndp - shift[0], ndp), lax.rem(me + n - shift[1], n)

    def remote(src, dst, send, recv, to):
        return pltpu.make_async_remote_copy(
            src_ref=src, dst_ref=dst, send_sem=send, recv_sem=recv, device_id=to, device_id_type=MESH
        )

    loads = [
        pltpu.make_async_copy(src.at[0], dst, load_sem.at[i])
        for i, (src, dst) in enumerate(((q_hbm, q_s), (do_hbm, do_s), (o_hbm, o_s)))
    ]
    home = dp * n + me
    loads.append(
        pltpu.make_async_copy(
            layer_hbm.at[0, :, pl.ds(pl.multiple_of(home * feats, LANES), feats)], a_s.at[home], load_sem.at[3]
        )
    )

    barrier = pltpu.get_barrier_semaphore()
    x_mates = [lax.rem(chip + k, xs) * CORES + core for k in range(1, xs)]
    mates = x_mates + [chip * CORES + (1 - core)]
    for shift in others:
        to = peer(shift)
        pl.semaphore_signal(barrier, inc=1, device_id=(to[0], to[1], tp), device_id_type=MESH)
    for mate in mates:
        pl.semaphore_signal(barrier, inc=1, device_id=(dp, me, mate), device_id_type=MESH)

    own_copies = []
    for half in range(2):
        for which, (hbm, buf) in enumerate(((k_hbm, kbuf), (v_hbm, vbuf))):
            own_copies.append(
                pltpu.make_async_copy(
                    hbm.at[0, pl.ds(half * block, block)], buf.at[half, REACH - 1], own_sem.at[half, which]
                )
            )
    for copy in own_copies + loads[:3]:
        copy.start()
    pl.semaphore_wait(barrier, len(others) + len(mates))

    def kv_pair(half, to_half, step, to):
        return [
            remote(
                hbm.at[0, pl.ds(half * block, block)],
                buf.at[to_half, REACH - 1 - step],
                kv_send.at[half, step - 1, which],
                kv_recv.at[to_half, step - 1, which],
                (dp, to, tp),
            )
            for which, (hbm, buf) in enumerate(((k_hbm, kbuf), (v_hbm, vbuf)))
        ]

    def each_kv(half, step):
        target = blocks[half] + step
        to, to_half = place_of(target, n)
        inside = target <= 2 * n - 1
        return kv_pair(half, to_half, step, to), inside & (to != me), inside & (to == me)

    for step in range(1, REACH):
        for half in range(2):
            pair, away, here = each_kv(half, step)

            @pl.when(away)
            def _():
                for copy in pair:
                    copy.start()

            if half == 0:

                @pl.when(here)
                def _():
                    for which, (hbm, buf) in enumerate(((k_hbm, kbuf), (v_hbm, vbuf))):
                        copy = pltpu.make_async_copy(
                            hbm.at[0, pl.ds(0, block)], buf.at[1, REACH - 1 - step], own_sem.at[2, which]
                        )
                        copy.start()
                        copy.wait()

    def a_copy(shift, slot):
        to = peer(shift)
        index = to[0] * n + to[1]
        return remote(
            layer_hbm.at[0, pl.ds(own_row, strip), pl.ds(pl.multiple_of(index * feats, LANES), feats)],
            a_s.at[home, pl.ds(own_row, strip)],
            a_send.at[slot],
            a_recv.at[slot],
            (to[0], to[1], tp),
        )

    a_copies = [a_copy(shift, slot) for slot, shift in enumerate(others)]
    for copy in a_copies:
        copy.start()
    loads[3].start()

    lanes = lax.broadcasted_iota(jnp.int32, (1, LANES), 1)
    low = lanes < block
    lse_s[0] = lse_ref[0]
    lse_s[1] = pltpu.roll(lse_ref[0], block, 1)
    docs = jnp.broadcast_to(doc_ref[...].astype(F32), (8, doc_ref.shape[1]))
    seq = doc_ref.shape[1]
    key_index = lax.broadcasted_iota(jnp.int32, (span, 2 * LANES), 0)
    query_index = span - block + lax.rem(lax.broadcasted_iota(jnp.int32, (span, 2 * LANES), 1), block)
    for half in range(2):
        start = (blocks[half] - (REACH - 1)) * block
        rolled = pltpu.roll(docs, lax.rem(2 * seq - start, seq), 1)[:1]
        key_row = rolled[:, :span]
        tail = rolled[:, span - LANES : span]
        query_row = jnp.where(low, pltpu.roll(jnp.broadcast_to(tail, (8, LANES)), block, 1)[:1], tail)
        key_docs = jnp.broadcast_to(key_row, (2 * LANES, span)).T
        query_docs = jnp.concatenate([query_row, query_row], axis=1)
        live = (key_index <= query_index) & (key_index + start >= 0) & (key_docs == query_docs)
        bias_s[half] = jnp.where(live, 0.0, -1e30)
        for step in range(1, REACH):

            @pl.when(blocks[half] - step < 0)
            def _():
                kbuf[half, REACH - 1 - step] = jnp.zeros((block, width), BF16)
                vbuf[half, REACH - 1 - step] = jnp.zeros((block, width), BF16)

    for copy in loads[:3] + own_copies:
        copy.wait()

    ones = jnp.ones((8, 2 * HD), BF16)

    def grad_copy(half, step):
        key_block = blocks[half] - step
        to, to_half = place_of(key_block, n)
        copy = remote(
            send_s.at[half, step - 1],
            recv_s.at[to_half, step - 1],
            g_send.at[half, step - 1],
            g_recv.at[to_half, step - 1],
            (dp, to, tp),
        )
        return copy, (key_block >= 0) & (to != me)

    for half in range(2):
        for step in range(1, REACH):
            key_block = blocks[half] - step
            holder, _ = place_of(key_block, n)

            @pl.when((key_block >= 0) & (holder != me))
            def _():
                for which, buf in enumerate((kbuf, vbuf)):
                    slot = buf.at[half, REACH - 1 - step]
                    remote(slot, slot, kv_send.at[half, step - 1, which], kv_recv.at[half, step - 1, which], (dp, holder, tp)).wait_recv()

        def group_step(g, carry):
            columns = pl.ds(pl.multiple_of(g * HD, HD), HD)
            keys = kbuf[half, :, :, columns].reshape(span, HD)
            values = vbuf[half, :, :, columns].reshape(span, HD)
            grad_key = jnp.zeros((span, HD), F32)
            grad_value = jnp.zeros((span, HD), F32)
            for part in range(per_group // stack):
                first = g * per_group + part * stack

                def stacked(ref):
                    return jnp.concatenate(
                        [
                            ref[half * block : (half + 1) * block, pl.ds(pl.multiple_of((first + j) * HD, HD), HD)]
                            for j in range(stack)
                        ],
                        axis=0,
                    )

                queries, grads, outs = stacked(q_s), stacked(do_s), stacked(o_s)
                product = grads.astype(F32) * outs.astype(F32)
                upper = product.astype(BF16)
                lower = (product - upper.astype(F32)).astype(BF16)
                delta = contract(ones, jnp.concatenate([upper, lower], axis=1), ((1,), (1,)))[:1]
                lse = jnp.concatenate(
                    [
                        jnp.where(
                            low, lse_s[half, pl.ds(first + j, 1), :], lse_s[1 - half, pl.ds(first + j + 1, 1), :]
                        )
                        for j in range(0, stack, 2)
                    ],
                    axis=1,
                )
                scores = contract(keys, queries, ((1,), (1,)))
                probs = jnp.exp(scores * scale - lse + bias_s[half])
                grad_probs = contract(values, grads, ((1,), (1,)))
                grad_scores = (probs * (grad_probs - delta)).astype(BF16)
                grad_value += contract(probs.astype(BF16), grads, ((1,), (0,)))
                grad_key += contract(grad_scores, queries, ((1,), (0,)))
                grad_query = (contract(grad_scores, keys, ((0,), (0,))) * scale).astype(BF16)
                for j in range(stack):
                    dq_s[half * block : (half + 1) * block, pl.ds(pl.multiple_of((first + j) * HD, HD), HD)] = grad_query[
                        j * block : (j + 1) * block
                    ]
            dkv_s[:, columns] = grad_key * scale
            dkv_s[:, pl.ds(pl.multiple_of(width + g * HD, HD), HD)] = grad_value
            return carry

        lax.fori_loop(0, groups, group_step, 0)
        acc_s[half] = dkv_s[span - block :]
        for step in range(1, REACH):
            at = (REACH - 1 - step) * block
            send_s[half, step - 1] = dkv_s[at : at + block].astype(BF16)
        for step in range(1, REACH):
            copy, away = grad_copy(half, step)

            @pl.when(away)
            def _():
                copy.start()

    dq_out = pltpu.make_async_copy(dq_s, dq_hbm.at[0], out_sem.at[0])
    dq_out.start()

    x_copies, c_copies = [], []
    for slot, shift in enumerate(others):
        a_copies[slot].wait_recv()
        from_dp, from_ctx = source(shift)
        index = from_dp * n + from_ctx
        piece = a_s.at[index, pl.ds(own_row, strip)]
        for k, mate in enumerate(x_mates):
            copy = remote(piece, piece, x_send.at[slot, k], x_recv.at[slot, k], (dp, me, mate))
            copy.start()
            x_copies.append(copy)

    for half in range(2):
        for step in range(1, REACH):
            target = blocks[half] + step
            to, _ = place_of(target, n)

            @pl.when((target <= 2 * n - 1) & (to != me))
            def _():
                slot = recv_s.at[half, step - 1]
                remote(slot, slot, g_send.at[half, step - 1], g_recv.at[half, step - 1], (dp, to, tp)).wait_recv()
                acc_s[half] += recv_s[half, step - 1].astype(F32)

            if half == 0:

                @pl.when(to == me)
                def _():
                    acc_s[0] += send_s[1, step - 1].astype(F32)

    for half in range(2):
        dk_ref[0, half * block : (half + 1) * block] = acc_s[half, :, :width].astype(BF16)
        grad_value = acc_s[half, :, width:].astype(BF16)
        dv_ref[0, half * block : (half + 1) * block] = grad_value
        vg_s[home, half * block : (half + 1) * block] = grad_value

    def vg_copy(index, slot, to):
        return remote(vg_s.at[index], vg_s.at[index], vg_send.at[slot], vg_recv.at[slot], (to[0], to[1], tp))

    vg_copies = {}
    for shift in others:
        if 0 in shift:
            vg_copies[shift] = vg_copy(home, shift[0] * n + shift[1], peer(shift))
            vg_copies[shift].start()

    for slot, shift in enumerate(others):
        from_dp, from_ctx = source(shift)
        index = from_dp * n + from_ctx
        for k in range(xs - 1):
            x_copies[slot * (xs - 1) + k].wait_recv()
        piece = a_s.at[index, pl.ds(core_row, xs * strip)]
        copy = remote(piece, piece, c_send.at[slot], c_recv.at[slot], (dp, me, mates[-1]))
        copy.start()
        c_copies.append(copy)

    for b in range(1, n):
        vg_copies[(0, b)].wait_recv()
        from_ctx = lax.rem(me + n - b, n)
        for a in range(1, ndp):
            copy = vg_copy(dp * n + from_ctx, a * n + b, (lax.rem(dp + a, ndp), me))
            copy.start()
            vg_copies[(a, b)] = copy

    loads[3].wait()
    for slot in range(len(others)):
        c_copies[slot].wait_recv()

    def flip(s, carry):
        at_s[:, pl.ds(pl.multiple_of(s * rows, LANES), rows)] = a_s[s].T
        return carry

    lax.fori_loop(0, ndp * n, flip, 0)
    for shift in others:
        if shift[0] != 0:
            vg_copies[shift].wait_recv()
    token_scale = (ndp * seq) ** (-0.5)
    grads_all = vg_s[...].reshape(ndp * n * rows, width)
    tile = 2 * LANES

    def tile_copy(t):
        at = pl.ds(pl.multiple_of(t * tile, tile), tile)
        return pltpu.make_async_copy(w_s.at[at], w_hbm.at[at], out_sem.at[1 + t])

    for t in range(feats // tile):
        w_s[t * tile : (t + 1) * tile] = (
            contract(at_s[t * tile : (t + 1) * tile], grads_all, ((1,), (0,))) * token_scale
        )
        tile_copy(t).start()

    dq_out.wait()
    for t in range(feats // tile):
        tile_copy(t).wait()
    for copy in a_copies + x_copies + c_copies + list(vg_copies.values()):
        copy.wait_send()
    for half in range(2):
        for step in range(1, REACH):
            pair, away, _ = each_kv(half, step)

            @pl.when(away)
            def _():
                for copy in pair:
                    copy.wait_send()

            copy, away = grad_copy(half, step)

            @pl.when(away)
            def _():
                copy.wait_send()


def fused_body(sizes, layer_input, queries, key_heads, value_heads, attn_out, out_grad, log_sums, doc_ids):
    ndp, n, ntp = sizes
    rows, head_width = queries.shape[1:]
    width = key_heads.shape[2]
    block = rows // 2
    span = REACH * block
    peers = ndp * n
    feats = layer_input.shape[2] // peers
    xs = ntp // CORES
    hops = REACH - 1
    dma = pltpu.SemaphoreType.DMA
    hbm = pl.BlockSpec(memory_space=pl.ANY)
    vmem = pl.BlockSpec(memory_space=pltpu.VMEM)
    return pl.pallas_call(
        functools.partial(fused_kernel, sizes),
        out_shape=(
            jax.ShapeDtypeStruct(queries.shape, BF16),
            jax.ShapeDtypeStruct(key_heads.shape, BF16),
            jax.ShapeDtypeStruct(key_heads.shape, BF16),
            jax.ShapeDtypeStruct((feats, width), F32),
        ),
        in_specs=[hbm] * 6 + [vmem] * 2,
        out_specs=(hbm, vmem, vmem, hbm),
        scratch_shapes=[
            pltpu.VMEM((rows, head_width), BF16),
            pltpu.VMEM((rows, head_width), BF16),
            pltpu.VMEM((rows, head_width), BF16),
            pltpu.VMEM((rows, head_width), BF16),
            pltpu.VMEM((2, REACH, block, width), BF16),
            pltpu.VMEM((2, REACH, block, width), BF16),
            pltpu.VMEM((2, span, 2 * LANES), F32),
            pltpu.VMEM((2, head_width // HD, rows), F32),
            pltpu.VMEM((span, 2 * width), F32),
            pltpu.VMEM((2, block, 2 * width), F32),
            pltpu.VMEM((2, hops, block, 2 * width), BF16),
            pltpu.VMEM((2, hops, block, 2 * width), BF16),
            pltpu.VMEM((peers, rows, feats), BF16),
            pltpu.VMEM((feats, peers * rows), BF16),
            pltpu.VMEM((peers, rows, width), BF16),
            pltpu.VMEM((feats, width), F32),
            dma((4,)),
            dma((3, 2)),
            dma((2, hops, 2)),
            dma((2, hops, 2)),
            dma((2, hops)),
            dma((2, hops)),
            dma((peers - 1,)),
            dma((peers - 1,)),
            dma((peers - 1, xs - 1)),
            dma((peers - 1, xs - 1)),
            dma((peers - 1,)),
            dma((peers - 1,)),
            dma((peers,)),
            dma((peers,)),
            dma((1 + feats // (2 * LANES),)),
        ],
        compiler_params=pltpu.CompilerParams(
            collective_id=0, has_side_effects=True, vmem_limit_bytes=48 * 1024 * 1024
        ),
    )(layer_input, queries, key_heads, value_heads, attn_out, out_grad, log_sums, doc_ids)


def with_halo(cells, sides, width):
    for axis, dim in sides:
        count = lax.axis_size(axis)
        ends = count - 1
        head = lax.slice_in_dim(cells, 0, width, axis=dim)
        tail = lax.slice_in_dim(cells, cells.shape[dim] - width, cells.shape[dim], axis=dim)
        cells = jnp.concatenate(
            [
                lax.ppermute(tail, axis, [(i, (i + 1) % count) for i in range(ends)]),
                cells,
                lax.ppermute(head, axis, [((i + 1) % count, i) for i in range(ends)]),
            ],
            axis=dim,
        )
    return cells


def tile_terms(query_rows, grad_rows, lse_rows, row_delta, key_value, live_mask):
    groups = query_rows.shape[1]
    score_scale = HD ** (-0.5)
    key_rows = key_value[:, : groups * HD].reshape(-1, groups, HD)
    value_rows = key_value[:, groups * HD :].reshape(-1, groups, HD)
    scores = (
        jnp.einsum("qgrd,kgd->grqk", query_rows, key_rows, preferred_element_type=jnp.float32)
        * score_scale
    )
    soft_probs = jnp.where(live_mask, jnp.exp(scores - lse_rows[..., None]), 0.0)
    grad_value = jnp.einsum(
        "grqk,qgrd->kgd",
        soft_probs.astype(jnp.bfloat16),
        grad_rows,
        preferred_element_type=jnp.float32,
    )
    grad_probs = jnp.einsum(
        "qgrd,kgd->grqk", grad_rows, value_rows, preferred_element_type=jnp.float32
    )
    grad_scores = (soft_probs * (grad_probs - row_delta[..., None])).astype(jnp.bfloat16)
    grad_query = (
        jnp.einsum("grqk,kgd->qgrd", grad_scores, key_rows, preferred_element_type=jnp.float32)
        * score_scale
    )
    grad_key = (
        jnp.einsum("grqk,qgrd->kgd", grad_scores, query_rows, preferred_element_type=jnp.float32)
        * score_scale
    )
    key_count = key_value.shape[0]
    joined = jnp.concatenate(
        [grad_key.reshape(key_count, groups * HD), grad_value.reshape(key_count, groups * HD)],
        axis=1,
    )
    return (grad_query, joined)


def block_terms(
    reach_step,
    query_block,
    key_block,
    doc_seq,
    block_rows,
    query_rows,
    grad_rows,
    lse_rows,
    row_delta,
    key_value,
):
    query_doc = lax.dynamic_slice_in_dim(doc_seq, query_block * block_rows, block_rows)
    key_doc = lax.dynamic_slice_in_dim(doc_seq, jnp.maximum(key_block, 0) * block_rows, block_rows)
    offsets = jnp.arange(block_rows, dtype=jnp.int32)
    query_pos = query_block * block_rows + offsets
    key_pos = key_block * block_rows + offsets
    live_mask = (
        (key_pos[None, :] <= query_pos[:, None])
        & (key_doc[None, :] == query_doc[:, None])
        & (key_block >= 0)
    )
    operands = (query_rows, grad_rows, lse_rows, row_delta, key_value, live_mask)
    if reach_step == 0:
        return tile_terms(*operands)

    def compute(packed):
        return tile_terms(*packed)

    def skipped(packed):
        return (jnp.zeros(packed[0].shape, jnp.float32), jnp.zeros(packed[4].shape, jnp.float32))

    live_tile = (key_block >= 0) & (key_doc[block_rows - 1] == query_doc[0])
    return lax.cond(live_tile, compute, skipped, operands)


def body(layer_input, queries, key_heads, value_heads, attn_out, out_grad, log_sums, doc_ids):
    ctx_index = lax.axis_index("ctx")
    ctx_count = lax.axis_size("ctx")
    block_rows = queries.shape[1] // 2
    kv_width = key_heads.shape[2]
    groups = kv_width // HD
    head_count = queries.shape[2] // HD
    per_group = head_count // groups
    query_rows = queries[0].reshape(2, block_rows, groups, per_group, HD)
    grad_rows = out_grad[0].reshape(2, block_rows, groups, per_group, HD)
    out_rows = attn_out[0].reshape(2, block_rows, groups, per_group, HD)
    row_delta = jnp.sum(
        grad_rows.astype(jnp.float32) * out_rows.astype(jnp.float32), axis=-1
    ).transpose(0, 2, 3, 1)
    lse_rows = log_sums[0].reshape(groups, per_group, 2, block_rows).transpose(2, 0, 1, 3)
    doc_seq = doc_ids[0]
    own_blocks = (ctx_index, 2 * ctx_count - 1 - ctx_index)
    key_value = jnp.concatenate([key_heads[0], value_heads[0]], axis=1)
    current = (key_value[:block_rows], key_value[block_rows:])
    last_device = ctx_index == ctx_count - 1
    query_accum = [
        jnp.zeros(query_rows.shape[1:], jnp.float32),
        jnp.zeros(query_rows.shape[1:], jnp.float32),
    ]
    pieces = []
    for reach_step in range(REACH):
        if reach_step > 0:
            stacked = jnp.concatenate([current[1], current[0]], axis=0)
            padded = with_halo(stacked, (("ctx", 0),), block_rows)
            current = (
                padded[:block_rows],
                jnp.where(last_device, current[0], padded[3 * block_rows :]),
            )
        grad_terms = []
        for which_half in range(2):
            query_block = own_blocks[which_half]
            grad_query, joined = block_terms(
                reach_step,
                query_block,
                query_block - reach_step,
                doc_seq,
                block_rows,
                query_rows[which_half],
                grad_rows[which_half],
                lse_rows[which_half],
                row_delta[which_half],
                current[which_half],
            )
            query_accum[which_half] = query_accum[which_half] + grad_query
            grad_terms.append(joined)
        pieces.append(grad_terms)
    accum_first, accum_second = pieces[REACH - 1]
    for reach_step in range(REACH - 1, 0, -1):
        stacked = jnp.concatenate([accum_first, accum_second], axis=0)
        padded = with_halo(stacked, (("ctx", 0),), block_rows)
        accum_first, accum_second = (
            jnp.where(last_device, accum_second, padded[3 * block_rows :])
            + pieces[reach_step - 1][0],
            padded[:block_rows] + pieces[reach_step - 1][1],
        )
    kv_grad = jnp.concatenate([accum_first, accum_second], axis=0)
    key_grad = kv_grad[:, :kv_width].astype(jnp.bfloat16)
    value_grad = kv_grad[:, kv_width:].astype(jnp.bfloat16)
    query_grad = (
        jnp.concatenate(query_accum, axis=0)
        .reshape(1, 2 * block_rows, head_count * HD)
        .astype(jnp.bfloat16)
    )
    tokens = layer_input[0]
    weight_scale = (lax.axis_size("dp") * doc_seq.shape[0]) ** (-0.5)
    weight_grad = lax.psum_scatter(
        jnp.einsum("td,tc->dc", tokens, value_grad, preferred_element_type=jnp.float32)
        * weight_scale,
        ("dp", "ctx"),
        scatter_dimension=0,
        tiled=True,
    )
    return (query_grad, key_grad[None], value_grad[None], weight_grad)


def fits(mesh, queries_shape, layer_shape, seq):
    ndp, n, ntp = (mesh.shape[axis] for axis in ("dp", "ctx", "tp"))
    feats = layer_shape[2] // (ndp * n)
    rows = queries_shape[1] // n
    return (
        ndp * n <= 16
        and n >= REACH
        and ntp > CORES
        and ntp % CORES == 0
        and feats % (2 * LANES) == 0
        and rows == LANES
        and rows % (16 * ntp) == 0
        and seq % LANES == 0
    )


def solution(mesh):
    sizes = tuple(mesh.shape[axis] for axis in ("dp", "ctx", "tp"))
    in_specs = (
        P("dp", "ctx", None),
        P("dp", "ctx", "tp"),
        P("dp", "ctx", "tp"),
        P("dp", "ctx", "tp"),
        P("dp", "ctx", "tp"),
        P("dp", "ctx", "tp"),
        P("dp", "tp", "ctx"),
        P("dp", None),
    )
    out_specs = (
        P("dp", "ctx", "tp"),
        P("dp", "ctx", "tp"),
        P("dp", "ctx", "tp"),
        P(("dp", "ctx"), "tp"),
    )

    def run(layer_input, queries, *rest):
        fused = fits(mesh, queries.shape, layer_input.shape, rest[-1].shape[1])
        chosen = functools.partial(fused_body, sizes) if fused else body
        return jax.shard_map(chosen, mesh=mesh, in_specs=in_specs, out_specs=out_specs, check_vma=False)(
            layer_input, queries, *rest
        )

    return run
```

```python
import functools
import jax
import jax.numpy as jnp
from jax import lax
from jax.experimental import pallas as pl
from jax.experimental.pallas import tpu as pltpu
from jax.sharding import PartitionSpec as P

REACH = 4
HD = 128
LANES = 128
CORES = 2
EARLY = 7
MESH = pl.DeviceIdType.MESH
F32 = jnp.float32
BF16 = jnp.bfloat16


def contract(left, right, dims):
    return lax.dot_general(left, right, (dims, ((), ())), preferred_element_type=F32)


def place_of(block, count):
    return jnp.where(block < count, block, 2 * count - 1 - block), jnp.where(block < count, 0, 1)


def fused_kernel(
    sizes,
    layer_hbm,
    q_hbm,
    k_hbm,
    v_hbm,
    o_hbm,
    do_hbm,
    lse_hbm,
    doc_hbm,
    dq_ref,
    dk_ref,
    dv_ref,
    w_s,
    q_s,
    o_s,
    do_s,
    lse_in,
    doc_ref,
    kbuf,
    vbuf,
    bias_s,
    lse_s,
    dkv_s,
    acc_s,
    held_s,
    send_s,
    recv_s,
    a_s,
    at_s,
    vg_s,
    load_sem,
    own_sem,
    kv_send,
    kv_recv,
    g_send,
    g_recv,
    a_send,
    a_recv,
    x_send,
    x_recv,
    c_send,
    c_recv,
    vg_send,
    vg_recv,
):
    ndp, n, ntp = sizes
    dp, me, tp = lax.axis_index("dp"), lax.axis_index("ctx"), lax.axis_index("tp")
    rows = q_s.shape[0]
    block = rows // 2
    groups = k_hbm.shape[2] // HD
    per_group = q_s.shape[1] // HD // groups
    stack = 2 * LANES // block
    span = REACH * block
    width = groups * HD
    scale = HD ** (-0.5)
    feats = w_s.shape[0]
    xs = ntp // CORES
    core = lax.rem(tp, CORES)
    chip = tp // CORES
    strip = rows // ntp
    own_row = pl.multiple_of((core * xs + chip) * strip, strip)
    core_row = pl.multiple_of(core * xs * strip, strip)
    others = [(a, b) for a in range(ndp) for b in range(n) if (a, b) != (0, 0)]
    others.sort(key=lambda ab: (ab[1] != 0, ab[0] + min(ab[1], n - ab[1])))
    blocks = (me, 2 * n - 1 - me)

    def peer(shift):
        return lax.rem(dp + shift[0], ndp), lax.rem(me + shift[1], n)

    def source(shift):
        return lax.rem(dp + ndp - shift[0], ndp), lax.rem(me + n - shift[1], n)

    def remote(src, dst, send, recv, to):
        return pltpu.make_async_remote_copy(
            src_ref=src, dst_ref=dst, send_sem=send, recv_sem=recv, device_id=to, device_id_type=MESH
        )

    loads = [
        pltpu.make_async_copy(src.at[0], dst, load_sem.at[i])
        for i, (src, dst) in enumerate(((q_hbm, q_s), (do_hbm, do_s), (o_hbm, o_s)))
    ]
    small = [
        pltpu.make_async_copy(lse_hbm.at[0], lse_in, load_sem.at[4]),
        pltpu.make_async_copy(doc_hbm, doc_ref, load_sem.at[5]),
    ]
    home = dp * n + me
    loads.append(
        pltpu.make_async_copy(
            layer_hbm.at[0, :, pl.ds(pl.multiple_of(home * feats, LANES), feats)], a_s.at[home], load_sem.at[3]
        )
    )

    barrier = pltpu.get_barrier_semaphore()
    x_mates = [lax.rem(chip + k, xs) * CORES + core for k in range(1, xs)]
    mates = x_mates + [chip * CORES + (1 - core)]
    for shift in others:
        to = peer(shift)
        pl.semaphore_signal(barrier, inc=1, device_id=(to[0], to[1], tp), device_id_type=MESH)
    for mate in mates:
        pl.semaphore_signal(barrier, inc=1, device_id=(dp, me, mate), device_id_type=MESH)

    own_copies = []
    for half in range(2):
        for which, (hbm, buf) in enumerate(((k_hbm, kbuf), (v_hbm, vbuf))):
            own_copies.append(
                pltpu.make_async_copy(
                    hbm.at[0, pl.ds(half * block, block)], buf.at[half, REACH - 1], own_sem.at[half, which]
                )
            )
    for copy in small + own_copies + loads[:3]:
        copy.start()
    pl.semaphore_wait(barrier, len(others) + len(mates))

    def kv_pair(half, to_half, step, to):
        return [
            remote(
                hbm.at[0, pl.ds(half * block, block)],
                buf.at[to_half, REACH - 1 - step],
                kv_send.at[half, step - 1, which],
                kv_recv.at[to_half, step - 1, which],
                (dp, to, tp),
            )
            for which, (hbm, buf) in enumerate(((k_hbm, kbuf), (v_hbm, vbuf)))
        ]

    def here_copy(hbm, buf, step, which):
        return pltpu.make_async_copy(
            hbm.at[0, pl.ds(0, block)], buf.at[1, REACH - 1 - step], own_sem.at[1 + step, which]
        )

    def each_kv(half, step):
        target = blocks[half] + step
        to, to_half = place_of(target, n)
        inside = (target <= 2 * n - 1) & (target != n)
        return kv_pair(half, to_half, step, to), inside & (to != me), inside & (to == me)

    for step in range(1, REACH):
        for half in range(2):
            pair, away, here = each_kv(half, step)

            @pl.when(away)
            def _():
                for copy in pair:
                    copy.start()

            if half == 0:

                @pl.when(here)
                def _():
                    for which, (hbm, buf) in enumerate(((k_hbm, kbuf), (v_hbm, vbuf))):
                        here_copy(hbm, buf, step, which).start()

    def a_copy(shift, slot):
        to = peer(shift)
        index = to[0] * n + to[1]
        return remote(
            layer_hbm.at[0, pl.ds(own_row, strip), pl.ds(pl.multiple_of(index * feats, LANES), feats)],
            a_s.at[home, pl.ds(own_row, strip)],
            a_send.at[slot],
            a_recv.at[slot],
            (to[0], to[1], tp),
        )

    a_copies = [a_copy(shift, slot) for slot, shift in enumerate(others)]
    for copy in a_copies[:EARLY]:
        copy.start()
    loads[3].start()

    for copy in small:
        copy.wait()
    lanes = lax.broadcasted_iota(jnp.int32, (1, LANES), 1)
    low = lanes < block
    lse_s[0] = lse_in[...]
    lse_s[1] = pltpu.roll(lse_in[...], block, 1)
    docs = jnp.broadcast_to(doc_ref[...].astype(F32), (8, doc_ref.shape[1]))
    seq = doc_ref.shape[1]
    key_index = lax.broadcasted_iota(jnp.int32, (span, 2 * LANES), 0)
    query_index = span - block + lax.rem(lax.broadcasted_iota(jnp.int32, (span, 2 * LANES), 1), block)
    for half in range(2):
        start = (blocks[half] - (REACH - 1)) * block
        rolled = pltpu.roll(docs, lax.rem(2 * seq - start, seq), 1)[:1]
        key_row = rolled[:, :span]
        tail = rolled[:, span - LANES : span]
        query_row = jnp.where(low, pltpu.roll(jnp.broadcast_to(tail, (8, LANES)), block, 1)[:1], tail)
        key_docs = jnp.broadcast_to(key_row, (2 * LANES, span)).T
        query_docs = jnp.concatenate([query_row, query_row], axis=1)
        live = (key_index <= query_index) & (key_index + start >= 0) & (key_docs == query_docs)
        bias_s[half] = jnp.where(live, 0.0, -1e30)
        for step in range(1, REACH):

            @pl.when(blocks[half] - step < 0)
            def _():
                kbuf[half, REACH - 1 - step] = jnp.zeros((block, width), BF16)
                vbuf[half, REACH - 1 - step] = jnp.zeros((block, width), BF16)

    for copy in loads[:3] + own_copies:
        copy.wait()
    last = me == n - 1
    for step in range(1, REACH):
        here = each_kv(0, step)[2]

        @pl.when(here)
        def _():
            for which, (hbm, buf) in enumerate(((k_hbm, kbuf), (v_hbm, vbuf))):
                here_copy(hbm, buf, step, which).wait()


    ones = jnp.ones((8, 2 * HD), BF16)

    def grad_copy(half, step):
        key_block = blocks[half] - step
        to, to_half = place_of(key_block, n)
        copy = remote(
            send_s.at[half, step - 1],
            recv_s.at[to_half, step - 1],
            g_send.at[half, step - 1],
            g_recv.at[to_half, step - 1],
            (dp, to, tp),
        )
        away = (key_block >= 0) & (to != me)
        if half == 0 and step < REACH - 1:
            away &= key_block + step != n - 1
        return copy, away

    for half in range(2):
        for step in range(1, REACH):
            key_block = blocks[half] - step
            holder, _ = place_of(key_block, n)

            @pl.when((key_block >= 0) & (holder != me) & (blocks[half] != n))
            def _():
                for which, buf in enumerate((kbuf, vbuf)):
                    slot = buf.at[half, REACH - 1 - step]
                    remote(slot, slot, kv_send.at[half, step - 1, which], kv_recv.at[half, step - 1, which], (dp, holder, tp)).wait_recv()

        if half == 1:

            @pl.when(last)
            def _():
                for buf in (kbuf, vbuf):
                    for step in range(1, REACH):
                        buf[1, REACH - 1 - step] = buf[0, REACH - step]

        def group_step(g, carry):
            columns = pl.ds(pl.multiple_of(g * HD, HD), HD)
            keys = kbuf[half, :, :, columns].reshape(span, HD)
            values = vbuf[half, :, :, columns].reshape(span, HD)
            grad_key = jnp.zeros((span, HD), F32)
            grad_value = jnp.zeros((span, HD), F32)
            for part in range(per_group // stack):
                first = g * per_group + part * stack

                def stacked(ref):
                    return jnp.concatenate(
                        [
                            ref[half * block : (half + 1) * block, pl.ds(pl.multiple_of((first + j) * HD, HD), HD)]
                            for j in range(stack)
                        ],
                        axis=0,
                    )

                queries, grads, outs = stacked(q_s), stacked(do_s), stacked(o_s)
                product = grads.astype(F32) * outs.astype(F32)
                upper = product.astype(BF16)
                lower = (product - upper.astype(F32)).astype(BF16)
                delta = contract(ones, jnp.concatenate([upper, lower], axis=1), ((1,), (1,)))[:1]
                lse = jnp.concatenate(
                    [
                        jnp.where(
                            low, lse_s[half, pl.ds(first + j, 1), :], lse_s[1 - half, pl.ds(first + j + 1, 1), :]
                        )
                        for j in range(0, stack, 2)
                    ],
                    axis=1,
                )
                scores = contract(keys, queries, ((1,), (1,)))
                probs = jnp.exp(scores * scale - lse + bias_s[half])
                grad_probs = contract(values, grads, ((1,), (1,)))
                grad_scores = (probs * (grad_probs - delta)).astype(BF16)
                grad_value += contract(probs.astype(BF16), grads, ((1,), (0,)))
                grad_key += contract(grad_scores, queries, ((1,), (0,)))
                grad_query = (contract(grad_scores, keys, ((0,), (0,))) * scale).astype(BF16)
                for j in range(stack):
                    dq_ref[0, half * block : (half + 1) * block, pl.ds(pl.multiple_of((first + j) * HD, HD), HD)] = grad_query[
                        j * block : (j + 1) * block
                    ]
            dkv_s[:, columns] = grad_key * scale
            dkv_s[:, pl.ds(pl.multiple_of(width + g * HD, HD), HD)] = grad_value
            return carry

        lax.fori_loop(0, groups, group_step, 0)
        acc_s[half] = dkv_s[span - block :]
        for step in range(1, REACH):
            at = (REACH - 1 - step) * block
            send_s[half, step - 1] = dkv_s[at : at + block].astype(BF16)
            if half == 0 and step < REACH - 1:
                held_s[step - 1] = dkv_s[at : at + block]
            if half == 1 and step > 1:

                @pl.when(last)
                def _():
                    send_s[1, step - 1] = (dkv_s[at : at + block] + held_s[step - 2]).astype(BF16)

        for step in range(1, REACH):
            copy, away = grad_copy(half, step)

            @pl.when(away)
            def _():
                copy.start()

    for copy in a_copies[EARLY:]:
        copy.start()

    x_copies, c_copies = {}, {}

    def slot_of(shift):
        from_dp, from_ctx = source(shift)
        return from_dp * n + from_ctx

    def share_with_chips(slots):
        for slot in slots:
            a_copies[slot].wait_recv()
            piece = a_s.at[slot_of(others[slot]), pl.ds(own_row, strip)]
            for k, mate in enumerate(x_mates):
                x_copies[slot, k] = remote(piece, piece, x_send.at[slot, k], x_recv.at[slot, k], (dp, me, mate))
                x_copies[slot, k].start()

    def share_with_core(slots):
        for slot in slots:
            for k in range(xs - 1):
                x_copies[slot, k].wait_recv()
            piece = a_s.at[slot_of(others[slot]), pl.ds(core_row, xs * strip)]
            c_copies[slot] = remote(piece, piece, c_send.at[slot], c_recv.at[slot], (dp, me, mates[-1]))
            c_copies[slot].start()

    def flip(s):
        at_s[:, pl.ds(pl.multiple_of(s * rows, LANES), rows)] = a_s[s].T

    def flip_all(slots):
        for slot in slots:
            c_copies[slot].wait_recv()
        shifts = [others[slot] for slot in slots]
        for shift in shifts:
            flip(slot_of(shift))

    early, late = range(EARLY), range(EARLY, len(others))
    share_with_chips(early)
    loads[3].wait()
    flip(home)

    for half in range(2):
        for step in range(1, REACH):
            target = blocks[half] + step
            to, _ = place_of(target, n)

            arrives = (target <= 2 * n - 1) & (to != me)
            if step < REACH - 1:
                arrives &= target != n - 1

            @pl.when(arrives)
            def _():
                slot = recv_s.at[half, step - 1]
                remote(slot, slot, g_send.at[half, step - 1], g_recv.at[half, step - 1], (dp, to, tp)).wait_recv()
                acc_s[half] += recv_s[half, step - 1].astype(F32)

            if half == 0:

                @pl.when(to == me)
                def _():
                    acc_s[0] += send_s[1, step - 1].astype(F32)

    for half in range(2):
        dk_ref[0, half * block : (half + 1) * block] = acc_s[half, :, :width].astype(BF16)
        grad_value = acc_s[half, :, width:].astype(BF16)
        dv_ref[0, half * block : (half + 1) * block] = grad_value
        vg_s[home, half * block : (half + 1) * block] = grad_value

    def vg_copy(index, slot, to):
        return remote(vg_s.at[index], vg_s.at[index], vg_send.at[slot], vg_recv.at[slot], (to[0], to[1], tp))

    vg_copies = {}
    for shift in others:
        if 0 in shift:
            vg_copies[shift] = vg_copy(home, shift[0] * n + shift[1], peer(shift))
            vg_copies[shift].start()
    share_with_chips(late)
    share_with_core(early)
    near = sorted(range(1, n), key=lambda b: min(b, n - b))
    share_with_core(late)
    for b in near:
        vg_copies[(0, b)].wait_recv()
        from_ctx = lax.rem(me + n - b, n)
        for a in range(1, ndp):
            vg_copies[(a, b)] = vg_copy(dp * n + from_ctx, a * n + b, (lax.rem(dp + a, ndp), me))
            vg_copies[(a, b)].start()
    flip_all(early)
    flip_all(late)
    for shift in others:
        if shift[0] != 0:
            vg_copies[shift].wait_recv()
    token_scale = (ndp * seq) ** (-0.5)
    grads_all = vg_s[...].reshape(ndp * n * rows, width)
    tile = 2 * LANES

    for t in range(feats // tile):
        w_s[t * tile : (t + 1) * tile] = (
            contract(at_s[t * tile : (t + 1) * tile], grads_all, ((1,), (0,))) * token_scale
        )

    for copy in a_copies + list(x_copies.values()) + list(c_copies.values()) + list(vg_copies.values()):
        copy.wait_send()
    for half in range(2):
        for step in range(1, REACH):
            pair, away, _ = each_kv(half, step)

            @pl.when(away)
            def _():
                for copy in pair:
                    copy.wait_send()

            copy, away = grad_copy(half, step)

            @pl.when(away)
            def _():
                copy.wait_send()


def store_kernel(*refs):
    copies = [pltpu.make_async_copy(refs[i], refs[4 + i], refs[8].at[i]) for i in range(4)]
    for copy in copies:
        copy.start()
    for copy in copies:
        copy.wait()


def fused_body(sizes, layer_input, queries, key_heads, value_heads, attn_out, out_grad, log_sums, doc_ids):
    ndp, n, ntp = sizes
    rows, head_width = queries.shape[1:]
    width = key_heads.shape[2]
    block = rows // 2
    span = REACH * block
    peers = ndp * n
    feats = layer_input.shape[2] // peers
    xs = ntp // CORES
    hops = REACH - 1
    dma = pltpu.SemaphoreType.DMA
    hbm = pl.BlockSpec(memory_space=pltpu.HBM)
    vmem = pl.BlockSpec(memory_space=pltpu.VMEM)
    results = pl.pallas_call(
        functools.partial(fused_kernel, sizes),
        out_shape=(
            jax.ShapeDtypeStruct(queries.shape, BF16),
            jax.ShapeDtypeStruct(key_heads.shape, BF16),
            jax.ShapeDtypeStruct(key_heads.shape, BF16),
            jax.ShapeDtypeStruct((feats, width), F32),
        ),
        in_specs=[hbm] * 8,
        out_specs=(vmem,) * 4,
        scratch_shapes=[
            pltpu.VMEM((rows, head_width), BF16),
            pltpu.VMEM((rows, head_width), BF16),
            pltpu.VMEM((rows, head_width), BF16),
            pltpu.VMEM(log_sums.shape[1:], F32),
            pltpu.VMEM(doc_ids.shape, jnp.int32),
            pltpu.VMEM((2, REACH, block, width), BF16),
            pltpu.VMEM((2, REACH, block, width), BF16),
            pltpu.VMEM((2, span, 2 * LANES), F32),
            pltpu.VMEM((2, head_width // HD, rows), F32),
            pltpu.VMEM((span, 2 * width), F32),
            pltpu.VMEM((2, block, 2 * width), F32),
            pltpu.VMEM((hops - 1, block, 2 * width), F32),
            pltpu.VMEM((2, hops, block, 2 * width), BF16),
            pltpu.VMEM((2, hops, block, 2 * width), BF16),
            pltpu.VMEM((peers, rows, feats), BF16),
            pltpu.VMEM((feats, peers * rows), BF16),
            pltpu.VMEM((peers, rows, width), BF16),
            dma((6,)),
            dma((1 + REACH, 2)),
            dma((2, hops, 2)),
            dma((2, hops, 2)),
            dma((2, hops)),
            dma((2, hops)),
            dma((peers - 1,)),
            dma((peers - 1,)),
            dma((peers - 1, xs - 1)),
            dma((peers - 1, xs - 1)),
            dma((peers - 1,)),
            dma((peers - 1,)),
            dma((peers,)),
            dma((peers,)),
        ],
        compiler_params=pltpu.CompilerParams(
            collective_id=0, has_side_effects=True, vmem_limit_bytes=48 * 1024 * 1024
        ),
    )(*(pltpu.with_memory_space_constraint(x, pltpu.HBM) for x in (layer_input, queries, key_heads, value_heads, attn_out, out_grad, log_sums, doc_ids)))
    return pl.pallas_call(
        store_kernel,
        out_shape=[jax.ShapeDtypeStruct(result.shape, result.dtype) for result in results],
        in_specs=[pl.BlockSpec(memory_space=pl.ANY)] * 4,
        out_specs=[hbm] * 4,
        scratch_shapes=[dma((4,))],
        compiler_params=pltpu.CompilerParams(vmem_limit_bytes=1024 * 1024),
    )(*results)


def with_halo(cells, sides, width):
    for axis, dim in sides:
        count = lax.axis_size(axis)
        ends = count - 1
        head = lax.slice_in_dim(cells, 0, width, axis=dim)
        tail = lax.slice_in_dim(cells, cells.shape[dim] - width, cells.shape[dim], axis=dim)
        cells = jnp.concatenate(
            [
                lax.ppermute(tail, axis, [(i, (i + 1) % count) for i in range(ends)]),
                cells,
                lax.ppermute(head, axis, [((i + 1) % count, i) for i in range(ends)]),
            ],
            axis=dim,
        )
    return cells


def tile_terms(query_rows, grad_rows, lse_rows, row_delta, key_value, live_mask):
    groups = query_rows.shape[1]
    score_scale = HD ** (-0.5)
    key_rows = key_value[:, : groups * HD].reshape(-1, groups, HD)
    value_rows = key_value[:, groups * HD :].reshape(-1, groups, HD)
    scores = (
        jnp.einsum("qgrd,kgd->grqk", query_rows, key_rows, preferred_element_type=jnp.float32)
        * score_scale
    )
    soft_probs = jnp.where(live_mask, jnp.exp(scores - lse_rows[..., None]), 0.0)
    grad_value = jnp.einsum(
        "grqk,qgrd->kgd",
        soft_probs.astype(jnp.bfloat16),
        grad_rows,
        preferred_element_type=jnp.float32,
    )
    grad_probs = jnp.einsum(
        "qgrd,kgd->grqk", grad_rows, value_rows, preferred_element_type=jnp.float32
    )
    grad_scores = (soft_probs * (grad_probs - row_delta[..., None])).astype(jnp.bfloat16)
    grad_query = (
        jnp.einsum("grqk,kgd->qgrd", grad_scores, key_rows, preferred_element_type=jnp.float32)
        * score_scale
    )
    grad_key = (
        jnp.einsum("grqk,qgrd->kgd", grad_scores, query_rows, preferred_element_type=jnp.float32)
        * score_scale
    )
    key_count = key_value.shape[0]
    joined = jnp.concatenate(
        [grad_key.reshape(key_count, groups * HD), grad_value.reshape(key_count, groups * HD)],
        axis=1,
    )
    return (grad_query, joined)


def block_terms(
    reach_step,
    query_block,
    key_block,
    doc_seq,
    block_rows,
    query_rows,
    grad_rows,
    lse_rows,
    row_delta,
    key_value,
):
    query_doc = lax.dynamic_slice_in_dim(doc_seq, query_block * block_rows, block_rows)
    key_doc = lax.dynamic_slice_in_dim(doc_seq, jnp.maximum(key_block, 0) * block_rows, block_rows)
    offsets = jnp.arange(block_rows, dtype=jnp.int32)
    query_pos = query_block * block_rows + offsets
    key_pos = key_block * block_rows + offsets
    live_mask = (
        (key_pos[None, :] <= query_pos[:, None])
        & (key_doc[None, :] == query_doc[:, None])
        & (key_block >= 0)
    )
    operands = (query_rows, grad_rows, lse_rows, row_delta, key_value, live_mask)
    if reach_step == 0:
        return tile_terms(*operands)

    def compute(packed):
        return tile_terms(*packed)

    def skipped(packed):
        return (jnp.zeros(packed[0].shape, jnp.float32), jnp.zeros(packed[4].shape, jnp.float32))

    live_tile = (key_block >= 0) & (key_doc[block_rows - 1] == query_doc[0])
    return lax.cond(live_tile, compute, skipped, operands)


def body(layer_input, queries, key_heads, value_heads, attn_out, out_grad, log_sums, doc_ids):
    ctx_index = lax.axis_index("ctx")
    ctx_count = lax.axis_size("ctx")
    block_rows = queries.shape[1] // 2
    kv_width = key_heads.shape[2]
    groups = kv_width // HD
    head_count = queries.shape[2] // HD
    per_group = head_count // groups
    query_rows = queries[0].reshape(2, block_rows, groups, per_group, HD)
    grad_rows = out_grad[0].reshape(2, block_rows, groups, per_group, HD)
    out_rows = attn_out[0].reshape(2, block_rows, groups, per_group, HD)
    row_delta = jnp.sum(
        grad_rows.astype(jnp.float32) * out_rows.astype(jnp.float32), axis=-1
    ).transpose(0, 2, 3, 1)
    lse_rows = log_sums[0].reshape(groups, per_group, 2, block_rows).transpose(2, 0, 1, 3)
    doc_seq = doc_ids[0]
    own_blocks = (ctx_index, 2 * ctx_count - 1 - ctx_index)
    key_value = jnp.concatenate([key_heads[0], value_heads[0]], axis=1)
    current = (key_value[:block_rows], key_value[block_rows:])
    last_device = ctx_index == ctx_count - 1
    query_accum = [
        jnp.zeros(query_rows.shape[1:], jnp.float32),
        jnp.zeros(query_rows.shape[1:], jnp.float32),
    ]
    pieces = []
    for reach_step in range(REACH):
        if reach_step > 0:
            stacked = jnp.concatenate([current[1], current[0]], axis=0)
            padded = with_halo(stacked, (("ctx", 0),), block_rows)
            current = (
                padded[:block_rows],
                jnp.where(last_device, current[0], padded[3 * block_rows :]),
            )
        grad_terms = []
        for which_half in range(2):
            query_block = own_blocks[which_half]
            grad_query, joined = block_terms(
                reach_step,
                query_block,
                query_block - reach_step,
                doc_seq,
                block_rows,
                query_rows[which_half],
                grad_rows[which_half],
                lse_rows[which_half],
                row_delta[which_half],
                current[which_half],
            )
            query_accum[which_half] = query_accum[which_half] + grad_query
            grad_terms.append(joined)
        pieces.append(grad_terms)
    accum_first, accum_second = pieces[REACH - 1]
    for reach_step in range(REACH - 1, 0, -1):
        stacked = jnp.concatenate([accum_first, accum_second], axis=0)
        padded = with_halo(stacked, (("ctx", 0),), block_rows)
        accum_first, accum_second = (
            jnp.where(last_device, accum_second, padded[3 * block_rows :])
            + pieces[reach_step - 1][0],
            padded[:block_rows] + pieces[reach_step - 1][1],
        )
    kv_grad = jnp.concatenate([accum_first, accum_second], axis=0)
    key_grad = kv_grad[:, :kv_width].astype(jnp.bfloat16)
    value_grad = kv_grad[:, kv_width:].astype(jnp.bfloat16)
    query_grad = (
        jnp.concatenate(query_accum, axis=0)
        .reshape(1, 2 * block_rows, head_count * HD)
        .astype(jnp.bfloat16)
    )
    tokens = layer_input[0]
    weight_scale = (lax.axis_size("dp") * doc_seq.shape[0]) ** (-0.5)
    weight_grad = lax.psum_scatter(
        jnp.einsum("td,tc->dc", tokens, value_grad, preferred_element_type=jnp.float32)
        * weight_scale,
        ("dp", "ctx"),
        scatter_dimension=0,
        tiled=True,
    )
    return (query_grad, key_grad[None], value_grad[None], weight_grad)


def fits(mesh, queries_shape, layer_shape, seq):
    ndp, n, ntp = (mesh.shape[axis] for axis in ("dp", "ctx", "tp"))
    feats = layer_shape[2] // (ndp * n)
    rows = queries_shape[1] // n
    return (
        ndp * n <= 16
        and n >= REACH
        and ntp > CORES
        and ntp % CORES == 0
        and feats % (2 * LANES) == 0
        and rows == LANES
        and rows % (16 * ntp) == 0
        and seq % LANES == 0
    )


def solution(mesh):
    sizes = tuple(mesh.shape[axis] for axis in ("dp", "ctx", "tp"))
    in_specs = (
        P("dp", "ctx", None),
        P("dp", "ctx", "tp"),
        P("dp", "ctx", "tp"),
        P("dp", "ctx", "tp"),
        P("dp", "ctx", "tp"),
        P("dp", "ctx", "tp"),
        P("dp", "tp", "ctx"),
        P("dp", None),
    )
    out_specs = (
        P("dp", "ctx", "tp"),
        P("dp", "ctx", "tp"),
        P("dp", "ctx", "tp"),
        P(("dp", "ctx"), "tp"),
    )

    def run(layer_input, queries, *rest):
        fused = fits(mesh, queries.shape, layer_input.shape, rest[-1].shape[1])
        chosen = functools.partial(fused_body, sizes) if fused else body
        return jax.shard_map(chosen, mesh=mesh, in_specs=in_specs, out_specs=out_specs, check_vma=False)(
            layer_input, queries, *rest
        )

    return run
```
